32 devices in a mesh: seq: 8 (over z, x), head: 4 (over y, core).
Axes of the slice: x: 2, y: 2, z: 4, core: 2. Of those that a mesh axis runs over, the one named last changes fastest.
Arguments:
- queries: bfloat16 [4096, 4096], P('seq', 'head'), may hold values from -6 to 6
- keys: bfloat16 [4096, 4096], P('seq', 'head'), may hold values from -6 to 6
- values: bfloat16 [4096, 4096], P('seq', 'head'), may hold values from -6 to 6
- med_weight: float32 [2, 32, 4], P(None, 'head'), may hold values from -3 to 3
- coarse_weight: float32 [2, 32, 64], P(None, 'head'), may hold values from -0.75 to 0.75
- out_weight: bfloat16 [4096, 4096], P('head'), may hold values from -0.09375 to 0.09375
Outputs:
- mixed: bfloat16 [4096, 4096], P('seq', 'head')
The draws below stay inside these ranges and needn't reach their ends.
All inputs are finite; a program needn't handle non-finite values.
Results may differ from the reference program's by a relative error of at most 0.013.
Values may be sent and summed in bfloat16 or wider, within the bound.
A program may use at most 128 MiB of HBM per device.

```python
import math
import jax
import jax.numpy as jnp
from jax import lax

D = 4096
HEADS = 32
HEAD_DIM = 128
TOK_DEV = 512
WIN = 512
MED = 4
COARSE = 64
TOKENS = 4096
N_SEQ = 8
N_HEAD = 4


def draw_queries(key, part):
    noise_key = jax.random.fold_in(key, 11)
    draws_bulk = jnp.clip(jax.random.normal(noise_key, (TOKENS, HEADS * HEAD_DIM), jnp.float32), -6.0, 6.0)
    return draws_bulk.astype(jnp.bfloat16)


def draw_keys(key, part):
    noise_key = jax.random.fold_in(key, 23)
    draws_bulk = jnp.clip(jax.random.normal(noise_key, (TOKENS, HEADS * HEAD_DIM), jnp.float32), -6.0, 6.0)
    return draws_bulk.astype(jnp.bfloat16)


def block_levels(stream_key, dims, cuts, smallest, top_value):
    def one(dim, shards_of):
        steps = jax.random.uniform(jax.random.fold_in(jax.random.fold_in(stream_key, 6), dim), (shards_of,), jnp.float32, smallest / len(cuts), top_value / len(cuts))
        return jnp.repeat(jnp.exp(steps), dims[dim] // shards_of).reshape((-1,) + (1,) * (len(dims) - dim - 1))

    gain = one(*cuts[0])
    for cut in cuts[1:]:
        gain = gain * one(*cut)
    return gain


def normal_values(stream_key, extent, spread, reach, pieces=(), kind=jnp.bfloat16):
    values = spread * jax.random.normal(stream_key, extent, jnp.float32)
    if pieces:
        values = values * block_levels(stream_key, extent, pieces, -0.22, 0.18)
    return jnp.clip(values, -reach, reach).astype(kind)


def setup_inputs(seed: int = 0) -> dict:
    arg_keys = jax.random.split(jax.random.key(seed), 7)
    queries = draw_queries(jax.random.fold_in(arg_keys[6], 71), 0)
    keys = draw_keys(jax.random.fold_in(arg_keys[6], 71), 0)
    values = normal_values(arg_keys[2], (TOKENS, HEADS * HEAD_DIM), 1.0, 6.0, ((0, 8), (1, 4)))
    med_weight = normal_values(arg_keys[3], (2, HEADS, MED), MED ** -0.5, 3.0, ((1, 4),), jnp.float32)
    coarse_weight = normal_values(arg_keys[4], (2, HEADS, COARSE), COARSE ** -0.5, 0.75, ((1, 4),), jnp.float32)
    out_weight = normal_values(arg_keys[5], (HEADS * HEAD_DIM, D), (HEADS * HEAD_DIM) ** -0.5, 0.09375, ((0, 4),))
    return dict(queries=queries, keys=keys, values=values, med_weight=med_weight, coarse_weight=coarse_weight, out_weight=out_weight)


def summarize(tensor, weight, ratio):
    groups = tensor.shape[0] // ratio
    grouped = tensor.reshape(groups, ratio, tensor.shape[1], tensor.shape[2]).astype(jnp.float32)
    return jnp.einsum('jrhd,hr->jhd', grouped, weight.astype(jnp.float32)).astype(jnp.bfloat16)

def reference(queries, keys, values, med_weight, coarse_weight, out_weight):
    head_width = HEAD_DIM
    query3 = queries.reshape(TOKENS, HEADS, head_width)
    key3 = keys.reshape(TOKENS, HEADS, head_width)
    value3 = values.reshape(TOKENS, HEADS, head_width)
    med_keys = summarize(key3, med_weight[0], MED)
    med_values = summarize(value3, med_weight[1], MED)
    coarse_keys = summarize(key3, coarse_weight[0], COARSE)
    coarse_values = summarize(value3, coarse_weight[1], COARSE)
    per_med = TOK_DEV // MED
    per_coarse = TOK_DEV // COARSE
    group_width = HEADS * head_width // N_HEAD
    score_scale = 1.0 / math.sqrt(head_width)
    coarse_owner = jnp.arange(TOKENS // COARSE, dtype=jnp.int32) // per_coarse

    def one_block(position):
        first = position * TOK_DEV
        query_blk = lax.dynamic_slice_in_dim(query3, first, TOK_DEV, 0)
        edge_first = jnp.maximum(first - WIN, 0).astype(jnp.int32)
        key_list = [lax.dynamic_slice_in_dim(key3, first, TOK_DEV, 0), lax.dynamic_slice_in_dim(key3, edge_first, WIN, 0)]
        value_list = [lax.dynamic_slice_in_dim(value3, first, TOK_DEV, 0), lax.dynamic_slice_in_dim(value3, edge_first, WIN, 0)]
        place_list = [jnp.arange(TOK_DEV, dtype=jnp.int32), jnp.full((WIN,), -1, jnp.int32)]
        usable_list = [jnp.ones((TOK_DEV,), bool), jnp.broadcast_to(position >= 1, (WIN,))]
        for distance in (2, 3, 4):
            med_first = (jnp.maximum(position - distance, 0) * per_med).astype(jnp.int32)
            key_list.append(lax.dynamic_slice_in_dim(med_keys, med_first, per_med, 0))
            value_list.append(lax.dynamic_slice_in_dim(med_values, med_first, per_med, 0))
            place_list.append(jnp.full((per_med,), -1, jnp.int32))
            usable_list.append(jnp.broadcast_to(position >= distance, (per_med,)))
        key_list.append(coarse_keys)
        value_list.append(coarse_values)
        place_list.append(jnp.full((TOKENS // COARSE,), -1, jnp.int32))
        usable_list.append(coarse_owner <= position - 1)
        key_all = jnp.concatenate(key_list, 0)
        value_all = jnp.concatenate(value_list, 0)
        key_place = jnp.concatenate(place_list, 0)
        usable = jnp.concatenate(usable_list, 0)
        query_place = jnp.arange(TOK_DEV, dtype=jnp.int32)
        allowed = (key_place[None, :] <= query_place[:, None]) & usable[None, :]
        scores = jnp.einsum('qhd,khd->hqk', query_blk.astype(jnp.float32), key_all.astype(jnp.float32)) * score_scale
        scores = jnp.where(allowed[None], scores, -jnp.inf)
        row_peak = lax.optimization_barrier(jnp.max(scores, axis=-1, keepdims=True))
        exp_scores = jnp.exp(scores - row_peak)
        row_total = lax.optimization_barrier(jnp.sum(exp_scores, axis=-1))
        rounded = lax.optimization_barrier(exp_scores.astype(jnp.bfloat16)).astype(jnp.float32)
        weighted = jnp.einsum('hqk,khd->hqd', rounded, value_all.astype(jnp.float32))
        attention = (weighted / row_total[..., None]).astype(jnp.bfloat16)
        attention = attention.transpose(1, 0, 2).reshape(TOK_DEV, HEADS * head_width)
        mixed = jnp.zeros((TOK_DEV, D), jnp.float32)
        for member in range(N_HEAD):
            partial_sum = jnp.dot(attention[:, member * group_width:(member + 1) * group_width], out_weight[member * group_width:(member + 1) * group_width], preferred_element_type=jnp.float32)
            mixed = mixed + lax.optimization_barrier(partial_sum.astype(jnp.bfloat16)).astype(jnp.float32)
        return mixed.astype(jnp.bfloat16)
    blocks = lax.map(one_block, jnp.arange(N_SEQ, dtype=jnp.int32))
    return blocks.reshape(TOKENS, D)
```

```python
import functools
import math

import jax
import jax.numpy as jnp
from jax import lax
from jax.experimental import pallas as pl
from jax.experimental.pallas import tpu as pltpu
from jax.sharding import PartitionSpec as P

HEAD_DIM = 128
MED = 4
COARSE = 64
CHUNKS = 2
MESH = pl.DeviceIdType.MESH
F32 = jnp.float32
BF16 = jnp.bfloat16


def mm(a, b):
    return jnp.dot(a, b, preferred_element_type=F32)


def mm_nt(a, b):
    return lax.dot_general(a, b, (((1,), (1,)), ((), ())), preferred_element_type=F32)


def split(w):
    hi = w.astype(BF16)
    return hi, (w - hi.astype(F32)).astype(BF16)


def kernel(
    n_seq, n_head, q_hbm, k_hbm, v_hbm, wm_ref, wc_ref, w_hbm, out_ref,
    q_v, k_v, v_v, w_v, vt, q_in, oe_out, le_out, oe_in, le_in,
    med_own, med_in, c_own, c_in, ck, cvt, o_loc, m_loc, l_loc, attn,
    pair_out, pair_in, far_out, far_in, acc,
    ld_sem, q_ss, q_rs, oe_ss, oe_rs, le_ss, le_rs, med_ss, med_rs, c_ss, c_rs,
    pair_ss, pair_rs, far_ss, far_rs,
):
    tok, feat = q_v.shape
    heads = feat // HEAD_DIM
    chunk = tok // CHUNKS
    n_med = tok // MED
    n_coarse = tok // COARSE
    width = out_ref.shape[1]
    scale = 1.0 / math.sqrt(HEAD_DIM)
    pos = lax.axis_index("seq")
    hd = lax.axis_index("head")
    groups = n_head // 2
    grp = hd // 2
    core = lax.rem(hd, 2)
    mate = grp * 2 + (1 - core)

    def remote(src, dst, ss, rs, **dev):
        return pltpu.make_async_remote_copy(
            src_ref=src, dst_ref=dst, send_sem=ss, recv_sem=rs,
            device_id=dev, device_id_type=MESH,
        )

    def hs(h):
        return pl.ds(pl.multiple_of(h * HEAD_DIM, HEAD_DIM), HEAD_DIM)

    loads = [
        pltpu.make_async_copy(s, d, ld_sem.at[n])
        for n, (s, d) in enumerate(((k_hbm, k_v), (v_hbm, v_v), (q_hbm, q_v), (w_hbm, w_v)))
    ]
    for ld in loads:
        ld.start()

    barrier = pltpu.get_barrier_semaphore()

    @pl.loop(1, n_seq)
    def _(d):
        pl.semaphore_signal(
            barrier, inc=1, device_id={"seq": lax.rem(pos + d, n_seq)}, device_id_type=MESH
        )

    @pl.loop(1, n_head)
    def _(d):
        pl.semaphore_signal(
            barrier, inc=1, device_id={"head": lax.rem(hd + d, n_head)}, device_id_type=MESH
        )

    @pl.loop(0, n_seq)
    def _(o):
        @pl.when(o >= pos)
        def _():
            c_in[o] = jnp.zeros(c_in.shape[1:], BF16)

    for slot in range(3):
        @pl.when(pos < slot + 2)
        def _():
            med_in[slot] = jnp.zeros(med_in.shape[1:], BF16)

    @pl.when(pos == 0)
    def _():
        oe_in[...] = jnp.zeros_like(oe_in)
        le_in[...] = jnp.full_like(le_in, -jnp.inf)

    pl.semaphore_wait(barrier, n_seq - 1 + n_head - 1)

    def q_copy(i):
        rows = pl.ds(i * chunk, chunk)
        return remote(
            q_hbm.at[rows], q_in.at[i], q_ss.at[i], q_rs.at[i], seq=jnp.maximum(pos - 1, 0)
        )

    def oe_copy(i, h):
        return remote(
            oe_out.at[i, h], oe_in.at[i, h], oe_ss.at[i, h], oe_rs.at[i, h],
            seq=jnp.minimum(pos + 1, n_seq - 1),
        )

    def le_copy(i):
        return remote(
            le_out.at[i], le_in.at[i], le_ss.at[i], le_rs.at[i],
            seq=jnp.minimum(pos + 1, n_seq - 1),
        )

    def med_copy(slot):
        src = med_own if slot == 0 else med_in.at[0]
        step = (2, 1, 2)[slot]
        return remote(
            src, med_in.at[slot], med_ss.at[slot], med_rs.at[slot],
            seq=jnp.minimum(pos + step, n_seq - 1),
        )

    def c_copy(to):
        return remote(c_own, c_in.at[pos], c_ss.at[to], c_rs.at[pos], seq=to)

    has_prev = pos >= 1
    has_next = pos < n_seq - 1

    @pl.when(has_prev)
    def _():
        for i in range(CHUNKS):
            q_copy(i).start()

    loads[0].wait()
    loads[1].wait()

    @pl.loop(0, heads)
    def _(h):
        kh = k_v[:, hs(h)]
        vh = v_v[:, hs(h)]
        vth = vh.T
        vt[h] = vth
        row = lax.broadcasted_iota(jnp.int32, (n_med, tok), 0)
        col = lax.broadcasted_iota(jnp.int32, (n_med, tok), 1)
        pick = (col // MED) == row
        hi, lo = split(jnp.where(pick, wm_ref[h], 0.0))
        med_own[0, h] = (mm(hi, kh) + mm(lo, kh)).astype(BF16)
        hi, lo = split(jnp.where(pick, wm_ref[heads + h], 0.0))
        med_own[1, h] = (mm_nt(vth, hi) + mm_nt(vth, lo)).astype(BF16)
        row = lax.broadcasted_iota(jnp.int32, (2 * n_coarse, tok), 0)
        col = lax.broadcasted_iota(jnp.int32, (2 * n_coarse, tok), 1) // COARSE
        hi, lo = split(jnp.where(col == row, wc_ref[h], 0.0))
        hi2, lo2 = split(jnp.where(col + n_coarse == row, wc_ref[heads + h], 0.0))
        c_own[h] = (mm(hi, kh) + mm(lo, kh) + mm(hi2, vh) + mm(lo2, vh)).astype(BF16)

    @pl.when(pos + 2 < n_seq)
    def _():
        med_copy(0).start()

    @pl.loop(0, n_seq)
    def _(to):
        @pl.when(to > pos)
        def _():
            c_copy(to).start()

    def edge(i):
        @pl.when(has_next)
        def _():
            q_copy(i).wait_recv()

            @pl.loop(0, heads)
            def _(h):
                s = mm_nt(k_v[:, hs(h)], q_in[i, :, hs(h)])
                m = jnp.max(s, axis=0, keepdims=True)
                p = jnp.exp((s - m) * scale)
                total = jnp.sum(p, axis=0, keepdims=True)
                o = mm(vt[h], p.astype(BF16))
                oe_out[i, h] = (o / total).astype(BF16)
                le_out[i, h] = m * scale + jnp.log(total)
                oe_copy(i, h).start()

            le_copy(i).start()

    def local(i):
        keys = (i + 1) * chunk
        first = i * chunk

        @pl.loop(0, heads)
        def _(h):
            q = q_v[pl.ds(first, chunk), hs(h)]
            s = mm_nt(k_v[pl.ds(0, keys), hs(h)], q)
            key_at = lax.broadcasted_iota(jnp.int32, (keys, chunk), 0)
            query_at = lax.broadcasted_iota(jnp.int32, (keys, chunk), 1) + first
            parts = [(jnp.where(key_at <= query_at, s, -jnp.inf), vt[h, :, pl.ds(0, keys)])]
            for slot in range(3):
                s = mm_nt(med_in[slot, 0, h], q)
                parts.append((jnp.where(pos >= slot + 2, s, -jnp.inf), med_in[slot, 1, h]))
            s = mm_nt(ck[h], q)
            owner = lax.broadcasted_iota(jnp.int32, s.shape, 0) // n_coarse
            parts.append((jnp.where(owner < pos, s, -jnp.inf), cvt[h]))
            m = functools.reduce(
                jnp.maximum, [jnp.max(s, axis=0, keepdims=True) for s, _ in parts]
            )
            total = 0.0
            o = 0.0
            for s, vals in parts:
                p = jnp.exp((s - m) * scale)
                total = total + jnp.sum(p, axis=0, keepdims=True)
                o = o + mm(vals, p.astype(BF16))
            o_loc[i, h] = o
            m_loc[i, h] = m * scale
            l_loc[i, h] = total

    def combine(i):
        @pl.when(has_prev)
        def _():
            le_copy(i).wait_recv()

            @pl.loop(0, heads)
            def _(h):
                oe_copy(i, h).wait_recv()

        @pl.loop(0, heads)
        def _(h):
            lse = le_in[i, h]
            top = jnp.maximum(m_loc[i, h], lse)
            a = jnp.exp(m_loc[i, h] - top)
            e = jnp.exp(lse - top)
            inv = 1.0 / (l_loc[i, h] * a + e)
            o = o_loc[i, h] * (a * inv) + oe_in[i, h].astype(F32) * (e * inv)
            attn[i, :, hs(h)] = o.T.astype(BF16)

    tile = math.gcd(width, 512)

    def project(i, target, put):
        @pl.loop(0, width // tile)
        def _(j):
            cols = pl.ds(pl.multiple_of(target * width + j * tile, tile), tile)
            put(pl.ds(pl.multiple_of(j * tile, tile), tile), mm(attn[i], w_v[:, cols]))

    def pair_copy(i, o):
        return remote(
            pair_out.at[i, o], pair_in.at[i, o], pair_ss.at[i, o], pair_rs.at[i, o], head=mate
        )

    def far_copy(i, o):
        return remote(
            far_out.at[i, o - 1], far_in.at[i, o - 1], far_ss.at[i, o - 1], far_rs.at[i, o - 1],
            head=lax.rem(grp + o, groups) * 2 + core,
        )

    def mix(i):
        order = list(range(1, groups)) + [0]
        for o in order:
            there = lax.rem(grp + o, groups) * 2

            def put_pair(cols, value):
                pair_out[i, o, :, cols] = value.astype(BF16)

            project(i, there + (1 - core), put_pair)
            pair_copy(i, o).start()
            if o:
                def put_far(cols, value):
                    acc[i, :, cols] = value

                project(i, there + core, put_far)
                pair_copy(i, o).wait_recv()
                far_out[i, o - 1] = (acc[i] + pair_in[i, o].astype(F32)).astype(BF16)
                far_copy(i, o).start()

        def put_own(cols, value):
            acc[i, :, cols] = value

        project(i, hd, put_own)

    edge(0)

    @pl.when(pos >= 2)
    def _():
        med_copy(0).wait_recv()

        @pl.when(has_next)
        def _():
            med_copy(1).start()

        @pl.when(pos + 2 < n_seq)
        def _():
            med_copy(2).start()

    for i in range(1, CHUNKS):
        edge(i)

    @pl.loop(0, n_seq)
    def _(o):
        @pl.when(o < pos)
        def _():
            remote(c_own, c_in.at[o], c_ss.at[o], c_rs.at[o], seq=o).wait_recv()

    @pl.loop(0, heads)
    def _(h):
        got = c_in[:, h].astype(F32)
        ck[h] = got[:, :n_coarse].reshape(n_seq * n_coarse, HEAD_DIM).astype(BF16)
        cvt[h] = got[:, n_coarse:].reshape(n_seq * n_coarse, HEAD_DIM).T.astype(BF16)

    loads[2].wait()
    for slot in (1, 2):
        @pl.when(pos >= slot + 2)
        def _():
            med_copy(slot).wait_recv()

    for i in range(CHUNKS):
        local(i)
    loads[3].wait()
    for i in range(CHUNKS):
        combine(i)
        mix(i)
    for i in range(CHUNKS):
        pair_copy(i, 0).wait_recv()
        total = acc[i] + pair_in[i, 0].astype(F32)
        for o in range(1, groups):
            far_copy(i, o).wait_recv()
            total = total + far_in[i, o - 1].astype(F32)
        out_ref[pl.ds(i * chunk, chunk), :] = total.astype(BF16)

    @pl.when(has_prev)
    def _():
        for i in range(CHUNKS):
            q_copy(i).wait_send()

    @pl.when(has_next)
    def _():
        for i in range(CHUNKS):
            le_copy(i).wait_send()

            @pl.loop(0, heads)
            def _(h):
                oe_copy(i, h).wait_send()

    @pl.when(pos + 2 < n_seq)
    def _():
        med_copy(0).wait_send()

    @pl.when((pos >= 2) & has_next)
    def _():
        med_copy(1).wait_send()

    @pl.when((pos >= 2) & (pos + 2 < n_seq))
    def _():
        med_copy(2).wait_send()

    @pl.loop(0, n_seq)
    def _(to):
        @pl.when(to > pos)
        def _():
            c_copy(to).wait_send()

    for i in range(CHUNKS):
        for o in range(groups):
            pair_copy(i, o).wait_send()
            if o:
                far_copy(i, o).wait_send()


def body(n_seq, n_head, queries, keys, values, med_weight, coarse_weight, out_weight):
    tok, feat = queries.shape
    heads = feat // HEAD_DIM
    chunk = tok // CHUNKS
    width = out_weight.shape[1] // n_head
    groups = n_head // 2
    far = max(groups - 1, 1)
    n_med = tok // MED
    n_coarse = tok // COARSE
    wm = jnp.tile(med_weight, (1, 1, n_med)).reshape(2 * heads, 1, tok)
    wc = jnp.tile(coarse_weight, (1, 1, n_coarse)).reshape(2 * heads, 1, tok)
    dma = pltpu.SemaphoreType.DMA
    hbm = pl.BlockSpec(memory_space=pl.ANY)
    vmem = pl.BlockSpec(memory_space=pltpu.VMEM)
    V = pltpu.VMEM
    scratch = [
        V((tok, feat), BF16), V((tok, feat), BF16), V((tok, feat), BF16),
        V(out_weight.shape, BF16),
        V((heads, HEAD_DIM, tok), BF16),
        V((CHUNKS, chunk, feat), BF16),
        V((CHUNKS, heads, HEAD_DIM, chunk), BF16),
        V((CHUNKS, heads, 1, chunk), F32),
        V((CHUNKS, heads, HEAD_DIM, chunk), BF16),
        V((CHUNKS, heads, 1, chunk), F32),
        V((2, heads, n_med, HEAD_DIM), BF16),
        V((3, 2, heads, n_med, HEAD_DIM), BF16),
        V((heads, 2 * n_coarse, HEAD_DIM), BF16),
        V((n_seq, heads, 2 * n_coarse, HEAD_DIM), BF16),
        V((heads, n_seq * n_coarse, HEAD_DIM), BF16),
        V((heads, HEAD_DIM, n_seq * n_coarse), BF16),
        V((CHUNKS, heads, HEAD_DIM, chunk), F32),
        V((CHUNKS, heads, 1, chunk), F32),
        V((CHUNKS, heads, 1, chunk), F32),
        V((CHUNKS, chunk, feat), BF16),
        V((CHUNKS, groups, chunk, width), BF16),
        V((CHUNKS, groups, chunk, width), BF16),
        V((CHUNKS, far, chunk, width), BF16),
        V((CHUNKS, far, chunk, width), BF16),
        V((CHUNKS, chunk, width), F32),
        dma((4,)),
        dma((CHUNKS,)), dma((CHUNKS,)),
        dma((CHUNKS, heads)), dma((CHUNKS, heads)),
        dma((CHUNKS,)), dma((CHUNKS,)),
        dma((3,)), dma((3,)),
        dma((n_seq,)), dma((n_seq,)),
        dma((CHUNKS, groups)), dma((CHUNKS, groups)),
        dma((CHUNKS, far)), dma((CHUNKS, far)),
    ]
    return pl.pallas_call(
        functools.partial(kernel, n_seq, n_head),
        out_shape=jax.ShapeDtypeStruct((tok, width), BF16),
        in_specs=[hbm, hbm, hbm, vmem, vmem, hbm],
        out_specs=vmem,
        scratch_shapes=scratch,
        compiler_params=pltpu.CompilerParams(
            collective_id=0, has_side_effects=True, vmem_limit_bytes=60 * 1024 * 1024
        ),
    )(queries, keys, values, wm, wc, out_weight)


def solution(mesh):
    placed = (
        P("seq", "head"),
        P("seq", "head"),
        P("seq", "head"),
        P(None, "head", None),
        P(None, "head", None),
        P("head", None),
    )
    return jax.shard_map(
        functools.partial(body, mesh.shape["seq"], mesh.shape["head"]),
        mesh=mesh, in_specs=placed, out_specs=P("seq", "head"), check_vma=False,
    )
```

```python
import functools
import math

import jax
import jax.numpy as jnp
from jax import lax
from jax.experimental import pallas as pl
from jax.experimental.pallas import tpu as pltpu
from jax.sharding import PartitionSpec as P

HEAD_DIM = 128
MED = 4
COARSE = 64
CHUNKS = 2
MESH = pl.DeviceIdType.MESH
F32 = jnp.float32
BF16 = jnp.bfloat16


def mm(a, b):
    return jnp.dot(a, b, preferred_element_type=F32)


def mm_nt(a, b):
    return lax.dot_general(a, b, (((1,), (1,)), ((), ())), preferred_element_type=F32)


def split(w):
    hi = w.astype(BF16)
    return hi, (w - hi.astype(F32)).astype(BF16)


def kernel(
    n_seq, n_head, q_hbm, k_hbm, v_hbm, wm_ref, wc_ref, w_hbm, out_ref,
    q_v, k_v, v_v, w_v, vt, q_in, oe_out, le_out, oe_in, le_in,
    med_own, med_in, c_own, c_in, ck, cvt, o_loc, m_loc, l_loc, attn,
    pair_out, pair_in, far_out, far_in, acc,
    ld_sem, q_ss, q_rs, oe_ss, oe_rs, le_ss, le_rs, med_ss, med_rs, c_ss, c_rs,
    pair_ss, pair_rs, far_ss, far_rs,
):
    tok, feat = q_v.shape
    heads = feat // HEAD_DIM
    chunk = tok // CHUNKS
    n_med = tok // MED
    n_coarse = tok // COARSE
    width = out_ref.shape[1]
    scale = 1.0 / math.sqrt(HEAD_DIM)
    pos = lax.axis_index("seq")
    hd = lax.axis_index("head")
    groups = n_head // 2
    grp = hd // 2
    core = lax.rem(hd, 2)
    mate = grp * 2 + (1 - core)

    def remote(src, dst, ss, rs, **dev):
        return pltpu.make_async_remote_copy(
            src_ref=src, dst_ref=dst, send_sem=ss, recv_sem=rs,
            device_id=dev, device_id_type=MESH,
        )

    def hs(h):
        return pl.ds(pl.multiple_of(h * HEAD_DIM, HEAD_DIM), HEAD_DIM)

    loads = [
        pltpu.make_async_copy(s, d, ld_sem.at[n])
        for n, (s, d) in enumerate(((k_hbm, k_v), (v_hbm, v_v), (q_hbm, q_v), (w_hbm, w_v)))
    ]
    for ld in loads:
        ld.start()

    barrier = pltpu.get_barrier_semaphore()

    @pl.loop(1, n_seq)
    def _(d):
        pl.semaphore_signal(
            barrier, inc=1, device_id={"seq": lax.rem(pos + d, n_seq)}, device_id_type=MESH
        )

    @pl.loop(1, n_head)
    def _(d):
        pl.semaphore_signal(
            barrier, inc=1, device_id={"head": lax.rem(hd + d, n_head)}, device_id_type=MESH
        )

    @pl.loop(0, n_seq)
    def _(o):
        @pl.when(o >= pos)
        def _():
            c_in[o] = jnp.zeros(c_in.shape[1:], BF16)

    for slot in range(2):
        @pl.when(pos < 2 * slot + 2)
        def _():
            med_in[slot] = jnp.zeros(med_in.shape[1:], BF16)

    @pl.when(pos == 0)
    def _():
        oe_in[...] = jnp.zeros_like(oe_in)
        le_in[...] = jnp.full_like(le_in, -jnp.inf)

    pl.semaphore_wait(barrier, n_seq - 1 + n_head - 1)

    def q_copy(i):
        rows = pl.ds(i * chunk, chunk)
        return remote(
            q_hbm.at[rows], q_in.at[i], q_ss.at[i], q_rs.at[i], seq=jnp.maximum(pos - 1, 0)
        )

    def oe_copy(i, h):
        return remote(
            oe_out.at[i, h], oe_in.at[i, h], oe_ss.at[i, h], oe_rs.at[i, h],
            seq=jnp.minimum(pos + 1, n_seq - 1),
        )

    def le_copy(i):
        return remote(
            le_out.at[i], le_in.at[i], le_ss.at[i], le_rs.at[i],
            seq=jnp.minimum(pos + 1, n_seq - 1),
        )

    def med_copy(slot):
        src = med_own if slot == 0 else med_in.at[0]
        return remote(
            src, med_in.at[slot], med_ss.at[slot], med_rs.at[slot],
            seq=jnp.minimum(pos + 2, n_seq - 1),
        )

    def c_copy(to):
        return remote(c_own, c_in.at[pos], c_ss.at[to], c_rs.at[pos], seq=to)

    has_prev = pos >= 1
    has_next = pos < n_seq - 1

    @pl.when(has_prev)
    def _():
        for i in range(CHUNKS):
            q_copy(i).start()

    loads[0].wait()
    loads[1].wait()

    @pl.loop(0, heads)
    def _(h):
        kh = k_v[:, hs(h)]
        vh = v_v[:, hs(h)]
        vth = vh.T
        vt[h] = vth
        row = lax.broadcasted_iota(jnp.int32, (n_med, tok), 0)
        col = lax.broadcasted_iota(jnp.int32, (n_med, tok), 1)
        pick = (col // MED) == row
        hi, lo = split(jnp.where(pick, wm_ref[h], 0.0))
        med_own[0, h] = (mm(hi, kh) + mm(lo, kh)).astype(BF16)
        hi, lo = split(jnp.where(pick, wm_ref[heads + h], 0.0))
        med_own[1, h] = (mm_nt(vth, hi) + mm_nt(vth, lo)).astype(BF16)
        row = lax.broadcasted_iota(jnp.int32, (2 * n_coarse, tok), 0)
        col = lax.broadcasted_iota(jnp.int32, (2 * n_coarse, tok), 1) // COARSE
        hi, lo = split(jnp.where(col == row, wc_ref[h], 0.0))
        hi2, lo2 = split(jnp.where(col + n_coarse == row, wc_ref[heads + h], 0.0))
        c_own[h] = (mm(hi, kh) + mm(lo, kh) + mm(hi2, vh) + mm(lo2, vh)).astype(BF16)

    @pl.when(pos + 2 < n_seq)
    def _():
        med_copy(0).start()

    @pl.loop(0, n_seq)
    def _(to):
        @pl.when(to > pos)
        def _():
            c_copy(to).start()

    def edge(i):
        @pl.when(has_next)
        def _():
            q_copy(i).wait_recv()

            @pl.loop(0, heads)
            def _(h):
                q = q_in[i, :, hs(h)]
                s = mm_nt(k_v[:, hs(h)], q)
                s2 = jnp.where(pos >= 2, mm_nt(med_in[0, 0, h], q), -jnp.inf)
                m = jnp.maximum(
                    jnp.max(s, axis=0, keepdims=True), jnp.max(s2, axis=0, keepdims=True)
                )
                p = jnp.exp((s - m) * scale)
                p2 = jnp.exp((s2 - m) * scale)
                total = jnp.sum(p, axis=0, keepdims=True) + jnp.sum(p2, axis=0, keepdims=True)
                o = mm(vt[h], p.astype(BF16)) + mm(med_in[0, 1, h], p2.astype(BF16))
                oe_out[i, h] = (o / total).astype(BF16)
                le_out[i, h] = m * scale + jnp.log(total)
                oe_copy(i, h).start()

            le_copy(i).start()

    def local(i):
        keys = (i + 1) * chunk
        first = i * chunk

        @pl.loop(0, heads)
        def _(h):
            q = q_v[pl.ds(first, chunk), hs(h)]
            s = mm_nt(k_v[pl.ds(0, keys), hs(h)], q)
            key_at = lax.broadcasted_iota(jnp.int32, (keys, chunk), 0)
            query_at = lax.broadcasted_iota(jnp.int32, (keys, chunk), 1) + first
            parts = [(jnp.where(key_at <= query_at, s, -jnp.inf), vt[h, :, pl.ds(0, keys)])]
            for slot in range(2):
                s = mm_nt(med_in[slot, 0, h], q)
                parts.append((jnp.where(pos >= 2 * slot + 2, s, -jnp.inf), med_in[slot, 1, h]))
            s = mm_nt(ck[h], q)
            owner = lax.broadcasted_iota(jnp.int32, s.shape, 0) // n_coarse
            parts.append((jnp.where(owner < pos, s, -jnp.inf), cvt[h]))
            m = functools.reduce(
                jnp.maximum, [jnp.max(s, axis=0, keepdims=True) for s, _ in parts]
            )
            total = 0.0
            o = 0.0
            for s, vals in parts:
                p = jnp.exp((s - m) * scale)
                total = total + jnp.sum(p, axis=0, keepdims=True)
                o = o + mm(vals, p.astype(BF16))
            o_loc[i, h] = o
            m_loc[i, h] = m * scale
            l_loc[i, h] = total

    def combine(i):
        @pl.when(has_prev)
        def _():
            le_copy(i).wait_recv()

            @pl.loop(0, heads)
            def _(h):
                oe_copy(i, h).wait_recv()

        @pl.loop(0, heads)
        def _(h):
            lse = le_in[i, h]
            top = jnp.maximum(m_loc[i, h], lse)
            a = jnp.exp(m_loc[i, h] - top)
            e = jnp.exp(lse - top)
            inv = 1.0 / (l_loc[i, h] * a + e)
            o = o_loc[i, h] * (a * inv) + oe_in[i, h].astype(F32) * (e * inv)
            attn[i, :, hs(h)] = o.T.astype(BF16)

    tile = math.gcd(width, 512)

    def project(i, target, put):
        @pl.loop(0, width // tile)
        def _(j):
            cols = pl.ds(pl.multiple_of(target * width + j * tile, tile), tile)
            put(pl.ds(pl.multiple_of(j * tile, tile), tile), mm(attn[i], w_v[:, cols]))

    def pair_copy(i, o):
        return remote(
            pair_out.at[i, o], pair_in.at[i, o], pair_ss.at[i, o], pair_rs.at[i, o], head=mate
        )

    def far_copy(i, o):
        return remote(
            far_out.at[i, o - 1], far_in.at[i, o - 1], far_ss.at[i, o - 1], far_rs.at[i, o - 1],
            head=lax.rem(grp + o, groups) * 2 + core,
        )

    def mix(i):
        order = list(range(1, groups)) + [0]
        for o in order:
            there = lax.rem(grp + o, groups) * 2

            def put_pair(cols, value):
                pair_out[i, o, :, cols] = value.astype(BF16)

            project(i, there + (1 - core), put_pair)
            pair_copy(i, o).start()
            if o:
                def put_far(cols, value):
                    acc[i, :, cols] = value

                project(i, there + core, put_far)
                pair_copy(i, o).wait_recv()
                far_out[i, o - 1] = (acc[i] + pair_in[i, o].astype(F32)).astype(BF16)
                far_copy(i, o).start()

        def put_own(cols, value):
            acc[i, :, cols] = value

        project(i, hd, put_own)

    @pl.when(pos >= 2)
    def _():
        med_copy(0).wait_recv()

        @pl.when(pos + 2 < n_seq)
        def _():
            med_copy(1).start()

    for i in range(CHUNKS):
        edge(i)

    @pl.loop(0, n_seq)
    def _(o):
        @pl.when(o < pos)
        def _():
            remote(c_own, c_in.at[o], c_ss.at[o], c_rs.at[o], seq=o).wait_recv()

    @pl.loop(0, heads)
    def _(h):
        got = c_in[:, h].astype(F32)
        ck[h] = got[:, :n_coarse].reshape(n_seq * n_coarse, HEAD_DIM).astype(BF16)
        cvt[h] = got[:, n_coarse:].reshape(n_seq * n_coarse, HEAD_DIM).T.astype(BF16)

    loads[2].wait()

    @pl.when(pos >= 4)
    def _():
        med_copy(1).wait_recv()

    loads[3].wait()
    for i in range(CHUNKS):
        local(i)
        combine(i)
        mix(i)
    for i in range(CHUNKS):
        pair_copy(i, 0).wait_recv()
        total = acc[i] + pair_in[i, 0].astype(F32)
        for o in range(1, groups):
            far_copy(i, o).wait_recv()
            total = total + far_in[i, o - 1].astype(F32)
        out_ref[pl.ds(i * chunk, chunk), :] = total.astype(BF16)

    @pl.when(has_prev)
    def _():
        for i in range(CHUNKS):
            q_copy(i).wait_send()

    @pl.when(has_next)
    def _():
        for i in range(CHUNKS):
            le_copy(i).wait_send()

            @pl.loop(0, heads)
            def _(h):
                oe_copy(i, h).wait_send()

    @pl.when(pos + 2 < n_seq)
    def _():
        med_copy(0).wait_send()

    @pl.when((pos >= 2) & (pos + 2 < n_seq))
    def _():
        med_copy(1).wait_send()

    @pl.loop(0, n_seq)
    def _(to):
        @pl.when(to > pos)
        def _():
            c_copy(to).wait_send()

    for i in range(CHUNKS):
        for o in range(groups):
            pair_copy(i, o).wait_send()
            if o:
                far_copy(i, o).wait_send()


def body(n_seq, n_head, queries, keys, values, med_weight, coarse_weight, out_weight):
    tok, feat = queries.shape
    heads = feat // HEAD_DIM
    chunk = tok // CHUNKS
    width = out_weight.shape[1] // n_head
    groups = n_head // 2
    far = max(groups - 1, 1)
    n_med = tok // MED
    n_coarse = tok // COARSE
    wm = jnp.tile(med_weight, (1, 1, n_med)).reshape(2 * heads, 1, tok)
    wc = jnp.tile(coarse_weight, (1, 1, n_coarse)).reshape(2 * heads, 1, tok)
    dma = pltpu.SemaphoreType.DMA
    hbm = pl.BlockSpec(memory_space=pl.ANY)
    vmem = pl.BlockSpec(memory_space=pltpu.VMEM)
    V = pltpu.VMEM
    scratch = [
        V((tok, feat), BF16), V((tok, feat), BF16), V((tok, feat), BF16),
        V(out_weight.shape, BF16),
        V((heads, HEAD_DIM, tok), BF16),
        V((CHUNKS, chunk, feat), BF16),
        V((CHUNKS, heads, HEAD_DIM, chunk), BF16),
        V((CHUNKS, heads, 1, chunk), F32),
        V((CHUNKS, heads, HEAD_DIM, chunk), BF16),
        V((CHUNKS, heads, 1, chunk), F32),
        V((2, heads, n_med, HEAD_DIM), BF16),
        V((2, 2, heads, n_med, HEAD_DIM), BF16),
        V((heads, 2 * n_coarse, HEAD_DIM), BF16),
        V((n_seq, heads, 2 * n_coarse, HEAD_DIM), BF16),
        V((heads, n_seq * n_coarse, HEAD_DIM), BF16),
        V((heads, HEAD_DIM, n_seq * n_coarse), BF16),
        V((CHUNKS, heads, HEAD_DIM, chunk), F32),
        V((CHUNKS, heads, 1, chunk), F32),
        V((CHUNKS, heads, 1, chunk), F32),
        V((CHUNKS, chunk, feat), BF16),
        V((CHUNKS, groups, chunk, width), BF16),
        V((CHUNKS, groups, chunk, width), BF16),
        V((CHUNKS, far, chunk, width), BF16),
        V((CHUNKS, far, chunk, width), BF16),
        V((CHUNKS, chunk, width), F32),
        dma((4,)),
        dma((CHUNKS,)), dma((CHUNKS,)),
        dma((CHUNKS, heads)), dma((CHUNKS, heads)),
        dma((CHUNKS,)), dma((CHUNKS,)),
        dma((2,)), dma((2,)),
        dma((n_seq,)), dma((n_seq,)),
        dma((CHUNKS, groups)), dma((CHUNKS, groups)),
        dma((CHUNKS, far)), dma((CHUNKS, far)),
    ]
    return pl.pallas_call(
        functools.partial(kernel, n_seq, n_head),
        out_shape=jax.ShapeDtypeStruct((tok, width), BF16),
        in_specs=[hbm, hbm, hbm, vmem, vmem, hbm],
        out_specs=vmem,
        scratch_shapes=scratch,
        compiler_params=pltpu.CompilerParams(
            collective_id=0, has_side_effects=True, vmem_limit_bytes=60 * 1024 * 1024
        ),
    )(queries, keys, values, wm, wc, out_weight)


def solution(mesh):
    placed = (
        P("seq", "head"),
        P("seq", "head"),
        P("seq", "head"),
        P(None, "head", None),
        P(None, "head", None),
        P("head", None),
    )
    return jax.shard_map(
        functools.partial(body, mesh.shape["seq"], mesh.shape["head"]),
        mesh=mesh, in_specs=placed, out_specs=P("seq", "head"), check_vma=False,
    )
```
